512 devices in a mesh: sub: 16 (over z, core), blk: 32 (over x, y).
Axes of the slice: x: 4, y: 8, z: 8, core: 2. Of those that a mesh axis runs over, the one named last changes fastest.
Arguments:
- double_layer: bfloat16 [16, 2, 2048, 2048], P('sub', None, 'blk'), may hold values from -1 to 2
- single_layer: bfloat16 [16, 2, 2048, 2048], P('sub', None, 'blk'), may hold values from -1 to 2
- hypersingular: bfloat16 [16, 2, 2048, 2048], P('sub', None, 'blk'), may hold values from -1 to 2
- adjoint_double: bfloat16 [16, 2, 2048, 2048], P('sub', None, 'blk'), may hold values from -1 to 2
- matching: int32 [16, 1024], replicated, may hold values from 0 to 1023, each once within a row
- right_side: float32 [16, 2, 2, 2048, 64], P('sub', None, None, 'blk'), may hold values from -6 to 6
- start: float32 [16, 2, 2, 2048, 64], P('sub', None, None, 'blk'), may hold values from -4 to 4
Outputs:
- solution: float32 [16, 2, 2, 2048, 64], P('sub', None, None, 'blk')
The draws below stay inside these ranges and needn't reach their ends.
Inputs may be any that keep to these rules, and one draw needn't show every extreme that they name: `matching`: each row is a permutation of 0 to 1023; row 0 pairs with no subdomain below and is not read.
All inputs are finite; a program needn't handle non-finite values.
Results may differ from the reference program's by a relative error of at most 0.015.
Values may be sent and summed in bfloat16 or wider, within the bound.
No kernel may reach another device: no remote copies, remote signals or barrier semaphores. Data moves between devices by JAX's collectives and lax.ppermute only.
A program may use at most 64 MiB of HBM per device.

```python
import math
import jax
import jax.numpy as jnp
from jax import lax

NH = 2048
RHS = 64
BASIS = 5
SUB = 16
HALF = 1024


def operator_block(key, salt):
    inner_key = jax.random.fold_in(key, salt)
    noise_key, diagonal_key = jax.random.split(inner_key)
    noise = jnp.clip(jax.random.normal(noise_key, (SUB, 2, NH, NH), jnp.float32), -2.0, 2.0) * (0.4 / math.sqrt(NH))
    diagonal = jax.random.uniform(diagonal_key, (SUB, NH), jnp.float32, 0.7, 1.3)
    identity = jnp.eye(NH, dtype=jnp.float32)
    real_part = noise[:, 0] + diagonal[:, :, None] * identity
    return jnp.stack([real_part, noise[:, 1]], axis=1).astype(jnp.bfloat16)


def draw_double_layer(key, part):
    return operator_block(key, 11)


def draw_single_layer(key, part):
    return operator_block(key, 23)


def draw_hypersingular(key, part):
    return operator_block(key, 37)


def draw_adjoint_double(key, part):
    return operator_block(key, 41)


def level_of(own_key, shape, cuts, least, top_value):
    def one(axis_at, blocks):
        steps = jax.random.uniform(jax.random.fold_in(jax.random.fold_in(own_key, 6), axis_at), (blocks,), jnp.float32, least / len(cuts), top_value / len(cuts))
        return jnp.repeat(jnp.exp(steps), shape[axis_at] // blocks).reshape((-1,) + (1,) * (len(shape) - axis_at - 1))

    gain = one(*cuts[0])
    for cut in cuts[1:]:
        gain = gain * one(*cut)
    return gain


def scatter_about(rng, dims, scale, reach, cuts=(), held_as=jnp.bfloat16):
    gain = level_of(rng, dims, cuts, -0.22, 0.18) if cuts else 1.0
    values = jax.random.normal(rng, dims, jnp.float32) * scale * gain
    return jnp.minimum(jnp.maximum(values, -reach), reach).astype(held_as)


def setup_inputs(seed: int = 0) -> dict:
    key_of = jax.random.split(jax.random.key(seed), 8)
    return {
        "double_layer": draw_double_layer(jax.random.fold_in(key_of[7], 71), 0),
        "single_layer": draw_single_layer(jax.random.fold_in(key_of[7], 71), 0),
        "hypersingular": draw_hypersingular(jax.random.fold_in(key_of[7], 71), 0),
        "adjoint_double": draw_adjoint_double(jax.random.fold_in(key_of[7], 71), 0),
        "matching": jax.vmap(lambda own: jax.random.permutation(own, HALF))(jax.random.split(key_of[4], SUB)).reshape((SUB, HALF)).astype(jnp.int32),
        "right_side": scatter_about(key_of[5], (SUB, 2, 2, NH, RHS), 1.0, 6.0, ((0, 16), (3, 32)), jnp.float32),
        "start": scatter_about(key_of[6], (SUB, 2, 2, NH, RHS), 0.5, 4.0, ((0, 16), (3, 32)), jnp.float32),
    }


EPSILON = 1e-06

def complex_product(matrix, vector):
    width = vector.shape[-1] // 2
    count = matrix.shape[1]
    products = jnp.dot(matrix.reshape(2 * count, matrix.shape[2]).astype(jnp.float32), vector.astype(jnp.float32), preferred_element_type=jnp.float32)
    products = products.reshape(2, count, 2 * width)
    real_part = products[0, :, :width] - products[1, :, width:]
    imag_part = products[0, :, width:] + products[1, :, :width]
    return jnp.concatenate([real_part, imag_part], axis=-1)

def calderon(double_layer, single_layer, hypersingular, adjoint_double, vector):
    upper = complex_product(single_layer, vector[1]) - complex_product(double_layer, vector[0])
    lower = complex_product(hypersingular, vector[0]) + complex_product(adjoint_double, vector[1])
    return jnp.stack([upper, lower])

def apply_all(operators, rounded):
    return lax.map(lambda pieces: calderon(*pieces), operators + (rounded,))

def take_rows(source, indices):
    return jnp.take(source, indices, axis=1)

def coupling(rounded, matching):
    odd_rows = rounded[:, :, 1::2]
    even_rows = rounded[:, :, 0::2]
    nothing = jnp.zeros_like(odd_rows[:1])
    odd_below = jnp.concatenate([nothing, odd_rows[:-1]], axis=0)
    even_above = jnp.concatenate([even_rows[1:], nothing], axis=0)
    inverse = jnp.argsort(matching, axis=1).astype(jnp.int32)
    inverse_above = jnp.concatenate([inverse[1:], inverse[:1]], axis=0)
    lower_face = jax.vmap(take_rows)(odd_below, matching)
    upper_face = jax.vmap(take_rows)(even_above, inverse_above)
    joined = jnp.stack([lower_face, upper_face], axis=3).reshape(rounded.shape).astype(jnp.float32)
    trace_signs = jnp.array([1.0, -1.0], jnp.float32).reshape(1, 2, 1, 1)
    return joined * trace_signs

def preconditioned(operators, matching, vector):
    rounded = vector.astype(jnp.bfloat16)
    middle = apply_all(operators, rounded) - 0.5 * coupling(rounded, matching)
    return apply_all(operators, middle.astype(jnp.bfloat16))

def inner(first, second):
    totals = lax.optimization_barrier(jnp.sum(first * second, axis=(0, 1, 2)))
    width = totals.shape[0] // 2
    return totals[:width] + totals[width:]

def spread(values):
    return jnp.concatenate([values, values])

def global_norm(vector):
    return jnp.sqrt(inner(vector, vector) + EPSILON)

def reference(double_layer, single_layer, hypersingular, adjoint_double, matching, right_side, start):
    operators = (double_layer, single_layer, hypersingular, adjoint_double)
    right_inner = jnp.concatenate([right_side[:, :, 0], right_side[:, :, 1]], axis=-1)
    start_inner = jnp.concatenate([start[:, :, 0], start[:, :, 1]], axis=-1)
    residual = right_inner - preconditioned(operators, matching, start_inner)
    beta = global_norm(residual)
    basis = [residual / spread(beta)]
    columns = []
    for column in range(BASIS):
        image = preconditioned(operators, matching, basis[column])
        coefficients = [inner(basis[earlier], image) for earlier in range(column + 1)]
        for earlier in range(column + 1):
            image = image - spread(coefficients[earlier]) * basis[earlier]
        height = global_norm(image)
        if column + 1 < BASIS:
            basis.append(image / spread(height))
        filler = [jnp.zeros_like(height)] * (BASIS - 1 - column)
        columns.append(jnp.stack(coefficients + [height] + filler, axis=1))
    hessen = jnp.stack(columns, axis=2)
    gram = jnp.einsum('rij,rik->rjk', hessen, hessen, precision=lax.Precision.HIGHEST)
    target = beta[:, None] * hessen[:, 0, :]
    factor = jnp.linalg.cholesky(gram)
    weights = jax.scipy.linalg.cho_solve((factor, True), target[..., None])[..., 0]
    solution = start_inner
    for column in range(BASIS):
        solution = solution + spread(weights[:, column]) * basis[column]
    width = solution.shape[-1] // 2
    return jnp.stack([solution[..., :width], solution[..., width:]], axis=2)
```

```python
import jax
import jax.numpy as jnp
from jax import lax
from jax.sharding import Mesh
from jax.sharding import PartitionSpec as P

BASIS = 5
SUB = ("sub_0", "sub_1")
BLK = ("blk_0", "blk_1")


EPSILON = 1e-06


def passed_along(block, axis, distance):
    devices = range(lax.axis_size(axis))
    route = [(i - distance, i) for i in devices if i - distance in devices]
    return lax.ppermute(block, axis, route)


def copy_for_each(value, axis):
    peers = lax.axis_size(axis)
    return lax.all_to_all(
        jnp.broadcast_to(value[None], (peers, *value.shape)), axis, 0, 0, tiled=True
    )


def summed_over(value, axis):
    return jnp.sum(copy_for_each(value, axis), axis=0)


def summed_everywhere(value):
    return summed_over(summed_over(value, SUB), BLK)


def inward(field):
    local_field = field[0]
    return jnp.concatenate([local_field[:, 0], local_field[:, 1]], axis=-1)


def outward(vector):
    width = vector.shape[-1] // 2
    return jnp.stack([vector[..., :width], vector[..., width:]], axis=1)[None]


def tile_of_operators(double_layer, single_layer, hypersingular, adjoint_double):
    columns = lax.axis_size("blk_0")
    grid = ((-double_layer, single_layer), (hypersingular, adjoint_double))
    traces = []
    for line in grid:
        pieces = []
        for part in range(2):
            for operator in line:
                rows, full = operator[part].shape
                pieces.append(
                    jnp.moveaxis(operator[part].reshape(rows, columns, full // columns), 1, 0)
                )
        traces.append(jnp.concatenate(pieces, axis=-1))
    strips = jnp.concatenate(traces, axis=1)
    blocks = lax.all_to_all(strips, "blk_0", 0, 0, tiled=True)
    return blocks.reshape(-1, blocks.shape[-1])


def selectors(matching, local_rows):
    subdomains = lax.axis_size(SUB)
    lines = lax.axis_size("blk_0")
    own_index = lax.axis_index(SUB)
    above_index = jnp.minimum(own_index + 1, subdomains - 1)
    perm_here = lax.dynamic_index_in_dim(matching, own_index, 0, keepdims=False)
    perm_above = lax.dynamic_index_in_dim(matching, above_index, 0, keepdims=False)
    half_rows = local_rows // 2
    half = perm_here.shape[0]
    spots = jnp.arange(half, dtype=jnp.int32)

    def window(values):
        table = values.reshape(lines, lax.axis_size("blk_1"), half_rows)
        return lax.dynamic_index_in_dim(
            table, lax.axis_index("blk_1"), 1, keepdims=False
        ).reshape(-1)

    wanted = window(spots)
    inverse_here = jnp.sum(
        jnp.where(perm_here[None, :] == wanted[:, None], spots[None, :], 0), axis=1
    )
    dofs = jnp.concatenate([2 * window(perm_above) + 1, 2 * inverse_here])
    width = 2 * half // lines
    columns = lax.axis_index("blk_0") * width + jnp.arange(width, dtype=jnp.int32)
    return (dofs[:, None] == columns[None, :]).astype(jnp.bfloat16)


def gathered_columns(vector):
    blocks = copy_for_each(vector, "blk_1")
    return jnp.moveaxis(blocks, 0, 1).reshape(
        vector.shape[0], blocks.shape[0] * vector.shape[1], vector.shape[2]
    )


def partial_products(tile, columns):
    width = columns.shape[-1] // 2
    turned = jnp.concatenate([-columns[..., width:], columns[..., :width]], axis=-1)
    stacked = jnp.stack([columns, turned]).reshape(tile.shape[1], 2 * width)
    products = jnp.dot(tile, stacked, preferred_element_type=jnp.float32)
    return products.reshape(lax.axis_size("blk_0"), 2, -1, 2 * width)


def coupling_partials(selector, columns):
    lines = lax.axis_size("blk_0")
    chosen = jnp.einsum(
        "sk,tkn->tsn", selector, columns, preferred_element_type=jnp.float32
    ).astype(jnp.bfloat16)
    middle = chosen.shape[1] // 2
    lower_face = passed_along(chosen[:, :middle], SUB, 1)
    upper_face = passed_along(chosen[:, middle:], SUB, -1)
    joined = jnp.stack([lower_face, upper_face], axis=2)
    joined = joined.reshape(2, lines, 2 * middle // lines, chosen.shape[-1])
    signs = jnp.array([1.0, -1.0], jnp.float32).reshape(1, 2, 1, 1)
    return jnp.moveaxis(joined, 1, 0).astype(jnp.float32) * signs


def reduced_rows(partials):
    return jnp.sum(lax.all_to_all(partials, "blk_0", 0, 0, tiled=True), axis=0)


def preconditioned(tile, selector, vector):
    columns = gathered_columns(vector.astype(jnp.bfloat16))
    first = partial_products(tile, columns) - 0.5 * coupling_partials(selector, columns)
    middle = reduced_rows(first)
    middle_columns = gathered_columns(middle.astype(jnp.bfloat16))
    return reduced_rows(partial_products(tile, middle_columns))


def inner_local(first, second):
    totals = jnp.sum(first * second, axis=(0, 1))
    width = totals.shape[0] // 2
    return totals[:width] + totals[width:]


def spread(values):
    return jnp.concatenate([values, values])


def least_squares(hessen, beta):
    gram = [
        [sum(a * b for a, b in zip(hessen[row], hessen[column])) for column in range(row + 1)]
        for row in range(BASIS)
    ]
    factor = [[None] * BASIS for _ in range(BASIS)]
    inverse = [None] * BASIS
    for row in range(BASIS):
        for column in range(row):
            rest = gram[row][column]
            for k in range(column):
                rest = rest - factor[row][k] * factor[column][k]
            factor[row][column] = rest * inverse[column]
        rest = gram[row][row]
        for k in range(row):
            rest = rest - factor[row][k] * factor[row][k]
        factor[row][row] = jnp.sqrt(rest)
        inverse[row] = 1.0 / factor[row][row]
    forward = []
    for row in range(BASIS):
        rest = beta * hessen[row][0]
        for k in range(row):
            rest = rest - factor[row][k] * forward[k]
        forward.append(rest * inverse[row])
    weights = [None] * BASIS
    for row in reversed(range(BASIS)):
        rest = forward[row]
        for k in range(row + 1, BASIS):
            rest = rest - factor[k][row] * weights[k]
        weights[row] = rest * inverse[row]
    return weights


def body(double_layer, single_layer, hypersingular, adjoint_double, matching, right_side, start):
    tile = tile_of_operators(
        double_layer[0], single_layer[0], hypersingular[0], adjoint_double[0]
    )
    right_local = inward(right_side)
    start_local = inward(start)
    selector = selectors(matching, right_local.shape[1])
    residual = right_local - preconditioned(tile, selector, start_local)
    beta = jnp.sqrt(summed_everywhere(inner_local(residual, residual)[None])[0] + EPSILON)
    basis = [residual / spread(beta)]
    hessen = []
    for column in range(BASIS):
        image = preconditioned(tile, selector, basis[column])
        local_dots = [inner_local(vector, image) for vector in basis]
        summed = summed_everywhere(jnp.stack(local_dots + [inner_local(image, image)]))
        squares = summed[column + 1] - jnp.sum(summed[: column + 1] * summed[: column + 1], axis=0)
        height = jnp.sqrt(jnp.maximum(squares, 0.0) + EPSILON)
        if column + 1 < BASIS:
            for earlier in range(column + 1):
                image = image - spread(summed[earlier]) * basis[earlier]
            basis.append(image / spread(height))
        filler = [jnp.zeros_like(height)] * (BASIS - 1 - column)
        hessen.append([summed[earlier] for earlier in range(column + 1)] + [height] + filler)
    weights = least_squares(hessen, beta)
    solution = start_local
    for column in range(BASIS):
        solution = solution + spread(weights[column]) * basis[column]
    return outward(solution)


def solution(mesh):
    torus = Mesh(mesh.devices.reshape(8, 2, 4, 8), ("sub_0", "sub_1", "blk_0", "blk_1"))
    placed = (
        P(SUB, None, BLK, None),
        P(SUB, None, BLK, None),
        P(SUB, None, BLK, None),
        P(SUB, None, BLK, None),
        P(),
        P(SUB, None, None, BLK, None),
        P(SUB, None, None, BLK, None),
    )
    return jax.shard_map(
        body, mesh=torus, in_specs=placed, out_specs=P(SUB, None, None, BLK, None), check_vma=False
    )
```

```python
import jax
import jax.numpy as jnp
from jax import lax
from jax.sharding import Mesh
from jax.sharding import PartitionSpec as P

BASIS = 5
SUB = ("sub_0", "sub_1")
BLK = ("blk_0", "blk_1")


EPSILON = 1e-06


def swapped_in_pairs(block, axis, first):
    devices = lax.axis_size(axis)
    route = []
    for low in range(first, devices - 1, 2):
        route += [(low, low + 1), (low + 1, low)]
    return lax.ppermute(block, axis, route)


def on_even_subdomain():
    return lax.axis_index(SUB) % 2 == 0


def copy_for_each(value, axis):
    peers = lax.axis_size(axis)
    return lax.all_to_all(
        jnp.broadcast_to(value[None], (peers, *value.shape)), axis, 0, 0, tiled=True
    )


def summed_over(value, axis):
    return jnp.sum(copy_for_each(value, axis), axis=0)


def summed_everywhere(value):
    return summed_over(summed_over(value, SUB), BLK)


def inward(field):
    local_field = field[0]
    return jnp.concatenate([local_field[:, 0], local_field[:, 1]], axis=-1)


def outward(vector):
    width = vector.shape[-1] // 2
    return jnp.stack([vector[..., :width], vector[..., width:]], axis=1)[None]


def tile_of_operators(double_layer, single_layer, hypersingular, adjoint_double):
    columns = lax.axis_size("blk_0")
    grid = ((-double_layer, single_layer), (hypersingular, adjoint_double))
    traces = []
    for line in grid:
        pieces = []
        for part in range(2):
            for operator in line:
                rows, full = operator[part].shape
                pieces.append(
                    jnp.moveaxis(operator[part].reshape(rows, columns, full // columns), 1, 0)
                )
        traces.append(jnp.concatenate(pieces, axis=-1))
    strips = jnp.concatenate(traces, axis=1)
    blocks = lax.all_to_all(strips, "blk_0", 0, 0, tiled=True)
    return blocks.reshape(-1, blocks.shape[-1])


def selectors(matching, local_rows):
    subdomains = lax.axis_size(SUB)
    lines = lax.axis_size("blk_0")
    own_index = lax.axis_index(SUB)
    above_index = jnp.minimum(own_index + 1, subdomains - 1)
    perm_here = lax.dynamic_index_in_dim(matching, own_index, 0, keepdims=False)
    perm_above = lax.dynamic_index_in_dim(matching, above_index, 0, keepdims=False)
    half_rows = local_rows // 2
    half = perm_here.shape[0]
    spots = jnp.arange(half, dtype=jnp.int32)

    def window(values):
        table = values.reshape(lines, lax.axis_size("blk_1"), half_rows)
        return lax.dynamic_index_in_dim(
            table, lax.axis_index("blk_1"), 1, keepdims=False
        ).reshape(-1)

    wanted = window(spots)
    inverse_here = jnp.sum(
        jnp.where(perm_here[None, :] == wanted[:, None], spots[None, :], 0), axis=1
    )
    upward = 2 * window(perm_above) + 1
    downward = 2 * inverse_here
    even = on_even_subdomain()
    dofs = jnp.concatenate(
        [jnp.where(even, upward, downward), jnp.where(even, downward, upward)]
    )
    width = 2 * half // lines
    columns = lax.axis_index("blk_0") * width + jnp.arange(width, dtype=jnp.int32)
    return (dofs[:, None] == columns[None, :]).astype(jnp.bfloat16)


def side_by_side(blocks):
    count, rows, width = blocks.shape
    return jnp.moveaxis(blocks.reshape(count, 2, rows // 2, width), 0, 1).reshape(
        2, count * rows // 2, width
    )


def partial_products(tile, columns):
    width = columns.shape[-1] // 2
    turned = jnp.concatenate([-columns[..., width:], columns[..., :width]], axis=-1)
    stacked = jnp.stack([columns, turned]).reshape(tile.shape[1], 2 * width)
    products = jnp.dot(tile, stacked, preferred_element_type=jnp.float32)
    return products.reshape(lax.axis_size("blk_0"), -1, 2 * width)


def coupling_partials(selector, columns):
    lines = lax.axis_size("blk_0")
    chosen = jnp.einsum(
        "sk,tkn->tsn", selector, columns, preferred_element_type=jnp.float32
    ).astype(jnp.bfloat16)
    middle = chosen.shape[1] // 2
    inner_face = swapped_in_pairs(chosen[:, :middle], SUB, 0)
    outer_face = swapped_in_pairs(chosen[:, middle:], SUB, 1)
    even = on_even_subdomain()
    lower_face = jnp.where(even, outer_face, inner_face)
    upper_face = jnp.where(even, inner_face, outer_face)
    joined = jnp.stack([lower_face, upper_face], axis=2)
    joined = joined.reshape(2, lines, 2 * middle // lines, chosen.shape[-1])
    signs = jnp.array([1.0, -1.0], jnp.float32).reshape(1, 2, 1, 1)
    signed = jnp.moveaxis(joined, 1, 0).astype(jnp.float32) * signs
    return signed.reshape(lines, -1, signed.shape[-1])


def reduced_rows(partials):
    return jnp.sum(lax.all_to_all(partials, "blk_0", 0, 0, tiled=True), axis=0)


def padded_rows(value, multiple):
    missing = -value.shape[0] % multiple
    return jnp.pad(value, ((0, missing), (0, 0)))


def in_three_pieces(value):
    high = lax.reduce_precision(value, 8, 7)
    middle = lax.reduce_precision(value - high, 8, 7)
    low = lax.reduce_precision(value - high - middle, 8, 7)
    return jnp.concatenate([high, middle, low]).astype(jnp.bfloat16)


def preconditioned(tile, selector, vector, dots=None):
    shape = vector.shape
    width = shape[-1]
    columns = side_by_side(
        copy_for_each(vector.astype(jnp.bfloat16).reshape(-1, width), "blk_1")
    )
    if dots is not None:
        dots = summed_over(dots, SUB)
    first = partial_products(tile, columns) - 0.5 * coupling_partials(selector, columns)
    middle = reduced_rows(first).astype(jnp.bfloat16)
    rows = middle.shape[0]
    if dots is None:
        middle_columns = side_by_side(copy_for_each(middle, "blk_1"))
        return reduced_rows(partial_products(tile, middle_columns)).reshape(shape)
    count, narrow = dots.shape
    packed = padded_rows(dots, 2).reshape(-1, width)
    lines = packed.shape[0]
    pieces = padded_rows(in_three_pieces(packed), 16)
    blocks = copy_for_each(jnp.concatenate([middle, pieces]), "blk_1")
    carried = blocks[:, rows : rows + 3 * lines].astype(jnp.float32)
    carried = jnp.sum(carried.reshape(-1, 3, lines, width), axis=(0, 1))
    second = partial_products(tile, side_by_side(blocks[:, :rows]))
    carried = jnp.broadcast_to(
        padded_rows(carried, 8)[None], (second.shape[0], lines + -lines % 8, width)
    )
    total = reduced_rows(jnp.concatenate([second, carried], axis=1))
    dots = total[rows : rows + lines].reshape(-1, narrow)[:count]
    return total[:rows].reshape(shape), dots


def inner_local(first, second):
    totals = jnp.sum(first * second, axis=(0, 1))
    width = totals.shape[0] // 2
    return totals[:width] + totals[width:]


def spread(values):
    return jnp.concatenate([values, values])


def least_squares(hessen, beta):
    gram = [
        [sum(a * b for a, b in zip(hessen[row], hessen[column])) for column in range(row + 1)]
        for row in range(BASIS)
    ]
    factor = [[None] * BASIS for _ in range(BASIS)]
    inverse = [None] * BASIS
    for row in range(BASIS):
        for column in range(row):
            rest = gram[row][column]
            for k in range(column):
                rest = rest - factor[row][k] * factor[column][k]
            factor[row][column] = rest * inverse[column]
        rest = gram[row][row]
        for k in range(row):
            rest = rest - factor[row][k] * factor[row][k]
        factor[row][row] = jnp.sqrt(rest)
        inverse[row] = 1.0 / factor[row][row]
    forward = []
    for row in range(BASIS):
        rest = beta * hessen[row][0]
        for k in range(row):
            rest = rest - factor[row][k] * forward[k]
        forward.append(rest * inverse[row])
    weights = [None] * BASIS
    for row in reversed(range(BASIS)):
        rest = forward[row]
        for k in range(row + 1, BASIS):
            rest = rest - factor[k][row] * weights[k]
        weights[row] = rest * inverse[row]
    return weights


def body(double_layer, single_layer, hypersingular, adjoint_double, matching, right_side, start):
    tile = tile_of_operators(
        double_layer[0], single_layer[0], hypersingular[0], adjoint_double[0]
    )
    right_local = inward(right_side)
    start_local = inward(start)
    selector = selectors(matching, right_local.shape[1])
    start_image = preconditioned(tile, selector, start_local)
    residual = right_local - start_image
    local_dots = jnp.stack(
        [
            inner_local(residual, residual),
            inner_local(start_local, start_image),
            inner_local(start_local, start_local),
        ]
    )
    applied, sums = preconditioned(tile, selector, residual, local_dots)
    beta = jnp.sqrt(sums[0] + EPSILON)
    shift = sums[1] / (sums[2] + EPSILON)
    basis = [residual / spread(beta)]
    images = [applied / spread(beta)]
    gram = (sums[0] / (beta * beta))[None, None]
    hessen = []
    for column in range(BASIS):
        ahead = images[column] - spread(shift) * basis[column]
        local_dots = [inner_local(vector, ahead) for vector in basis]
        local_dots = jnp.stack(local_dots + [inner_local(ahead, ahead)])
        if column + 1 < BASIS:
            applied, sums = preconditioned(tile, selector, ahead, local_dots)
        else:
            sums = summed_everywhere(local_dots)
        dots = sums[: column + 1]
        coefficients = dots + shift * gram[:, column]
        removed = jnp.concatenate([coefficients[:column], dots[column:] + shift * (gram[column:, column] - 1.0)])
        overlaps = jnp.sum(gram * removed[None], axis=1)
        squares = jnp.maximum(
            sums[column + 1] - jnp.sum(removed * (2.0 * dots - overlaps), axis=0), 0.0
        )
        height = jnp.sqrt(squares + EPSILON)
        if column + 1 < BASIS:
            following = ahead
            for earlier in range(column + 1):
                following = following - spread(removed[earlier]) * basis[earlier]
                applied = applied - spread(removed[earlier]) * images[earlier]
            basis.append(following / spread(height))
            images.append(applied / spread(height))
            side = (dots - overlaps) / height
            corner = squares / (height * height)
            gram = jnp.concatenate(
                [
                    jnp.concatenate([gram, side[:, None]], axis=1),
                    jnp.concatenate([side, corner[None]])[None],
                ]
            )
            shift = coefficients[column]
        filler = [jnp.zeros_like(height)] * (BASIS - 1 - column)
        hessen.append([coefficients[earlier] for earlier in range(column + 1)] + [height] + filler)
    weights = least_squares(hessen, beta)
    solution = start_local
    for column in range(BASIS):
        solution = solution + spread(weights[column]) * basis[column]
    return outward(solution)


def solution(mesh):
    torus = Mesh(mesh.devices.reshape(8, 2, 4, 8), ("sub_0", "sub_1", "blk_0", "blk_1"))
    placed = (
        P(SUB, None, BLK, None),
        P(SUB, None, BLK, None),
        P(SUB, None, BLK, None),
        P(SUB, None, BLK, None),
        P(),
        P(SUB, None, None, BLK, None),
        P(SUB, None, None, BLK, None),
    )
    return jax.shard_map(
        body, mesh=torus, in_specs=placed, out_specs=P(SUB, None, None, BLK, None), check_vma=False
    )
```

```python
import jax
import jax.numpy as jnp
from jax import lax
from jax.sharding import Mesh
from jax.sharding import PartitionSpec as P

BASIS = 5
SUB = ("sub_0", "sub_1")
BLK = ("blk_0", "blk_1")


EPSILON = 1e-06


def passed_along(block, axis, distance):
    devices = range(lax.axis_size(axis))
    route = [(i - distance, i) for i in devices if i - distance in devices]
    return lax.ppermute(block, axis, route)


def copy_for_each(value, axis):
    peers = lax.axis_size(axis)
    return lax.all_to_all(
        jnp.broadcast_to(value[None], (peers, *value.shape)), axis, 0, 0, tiled=True
    )


def summed_over(value, axis):
    return jnp.sum(copy_for_each(value, axis), axis=0)


def summed_everywhere(value):
    return summed_over(summed_over(value, SUB), BLK)


def inward(field):
    local_field = field[0]
    return jnp.concatenate([local_field[:, 0], local_field[:, 1]], axis=-1)


def outward(vector):
    width = vector.shape[-1] // 2
    return jnp.stack([vector[..., :width], vector[..., width:]], axis=1)[None]


def tile_of_operators(double_layer, single_layer, hypersingular, adjoint_double):
    columns = lax.axis_size("blk_0")
    grid = ((-double_layer, single_layer), (hypersingular, adjoint_double))
    traces = []
    for line in grid:
        pieces = []
        for part in range(2):
            for operator in line:
                rows, full = operator[part].shape
                pieces.append(
                    jnp.moveaxis(operator[part].reshape(rows, columns, full // columns), 1, 0)
                )
        traces.append(jnp.concatenate(pieces, axis=-1))
    strips = jnp.concatenate(traces, axis=1)
    blocks = lax.all_to_all(strips, "blk_0", 0, 0, tiled=True)
    return blocks.reshape(-1, blocks.shape[-1])


def selectors(matching, local_rows):
    subdomains = lax.axis_size(SUB)
    lines = lax.axis_size("blk_0")
    own_index = lax.axis_index(SUB)
    above_index = jnp.minimum(own_index + 1, subdomains - 1)
    perm_here = lax.dynamic_index_in_dim(matching, own_index, 0, keepdims=False)
    perm_above = lax.dynamic_index_in_dim(matching, above_index, 0, keepdims=False)
    half_rows = local_rows // 2
    half = perm_here.shape[0]
    spots = jnp.arange(half, dtype=jnp.int32)

    def window(values):
        table = values.reshape(lines, lax.axis_size("blk_1"), half_rows)
        return lax.dynamic_index_in_dim(
            table, lax.axis_index("blk_1"), 1, keepdims=False
        ).reshape(-1)

    wanted = window(spots)
    inverse_here = jnp.sum(
        jnp.where(perm_here[None, :] == wanted[:, None], spots[None, :], 0), axis=1
    )
    dofs = jnp.concatenate([2 * window(perm_above) + 1, 2 * inverse_here])
    width = 2 * half // lines
    columns = lax.axis_index("blk_0") * width + jnp.arange(width, dtype=jnp.int32)
    return (dofs[:, None] == columns[None, :]).astype(jnp.bfloat16)


def side_by_side(blocks):
    count, rows, width = blocks.shape
    return jnp.moveaxis(blocks.reshape(count, 2, rows // 2, width), 0, 1).reshape(
        2, count * rows // 2, width
    )


def partial_products(tile, columns):
    width = columns.shape[-1] // 2
    turned = jnp.concatenate([-columns[..., width:], columns[..., :width]], axis=-1)
    stacked = jnp.stack([columns, turned]).reshape(tile.shape[1], 2 * width)
    products = jnp.dot(tile, stacked, preferred_element_type=jnp.float32)
    return products.reshape(lax.axis_size("blk_0"), -1, 2 * width)


def coupling_partials(selector, columns):
    lines = lax.axis_size("blk_0")
    chosen = jnp.einsum(
        "sk,tkn->tsn", selector, columns, preferred_element_type=jnp.float32
    ).astype(jnp.bfloat16)
    middle = chosen.shape[1] // 2
    lower_face = passed_along(chosen[:, :middle], SUB, 1)
    upper_face = passed_along(chosen[:, middle:], SUB, -1)
    joined = jnp.stack([lower_face, upper_face], axis=2)
    joined = joined.reshape(2, lines, 2 * middle // lines, chosen.shape[-1])
    signs = jnp.array([1.0, -1.0], jnp.float32).reshape(1, 2, 1, 1)
    signed = jnp.moveaxis(joined, 1, 0).astype(jnp.float32) * signs
    return signed.reshape(lines, -1, signed.shape[-1])


def exchanged_rows(partials):
    return lax.all_to_all(partials, "blk_0", 0, 0, tiled=True).astype(jnp.float32)


def reduced_rows(partials):
    return jnp.sum(exchanged_rows(partials.astype(jnp.bfloat16)), axis=0)


def padded_rows(value, multiple):
    missing = -value.shape[0] % multiple
    return jnp.pad(value, ((0, missing), (0, 0)))


def in_three_pieces(value):
    high = lax.reduce_precision(value, 8, 7)
    middle = lax.reduce_precision(value - high, 8, 7)
    low = lax.reduce_precision(value - high - middle, 8, 7)
    return jnp.concatenate([high, middle, low]).astype(jnp.bfloat16)


def pieces_of(dots, width):
    packed = padded_rows(dots, 2).reshape(-1, width)
    return padded_rows(in_three_pieces(packed), 16)


def sum_of_pieces(blocks, lines):
    carried = blocks[:, : 3 * lines].astype(jnp.float32)
    return jnp.sum(carried.reshape(-1, 3, lines, carried.shape[-1]), axis=(0, 1))


def preconditioned(tile, selector, vector, dots=None):
    shape = vector.shape
    width = shape[-1]
    payload = vector.astype(jnp.bfloat16).reshape(-1, width)
    rows = payload.shape[0]
    if dots is not None:
        payload, dots = lax.optimization_barrier((payload, dots))
    blocks = copy_for_each(payload, "blk_1")
    if dots is not None:
        blocks, dots = lax.optimization_barrier((blocks, dots))
        dots = summed_over(dots, SUB)
    columns = side_by_side(blocks)
    first = partial_products(tile, columns) - 0.5 * coupling_partials(selector, columns)
    first = first.astype(jnp.bfloat16)
    if dots is None:
        middle = reduced_rows(first).astype(jnp.bfloat16)
        middle_columns = side_by_side(copy_for_each(middle, "blk_1"))
        return reduced_rows(partial_products(tile, middle_columns)).reshape(shape)
    count, narrow = dots.shape
    pieces = pieces_of(dots, width)
    lines = -(-count * narrow // width)
    first, pieces = lax.optimization_barrier((first, pieces))
    middle = reduced_rows(first).astype(jnp.bfloat16)
    blocks = copy_for_each(jnp.concatenate([middle, pieces]), "blk_1")
    second = partial_products(tile, side_by_side(blocks[:, :rows])).astype(jnp.bfloat16)
    carried = in_three_pieces(sum_of_pieces(blocks[:, rows:], lines))
    carried = padded_rows(carried, 16)
    carried = jnp.broadcast_to(carried[None], (second.shape[0], *carried.shape))
    exchanged = exchanged_rows(jnp.concatenate([second, carried], axis=1))
    image = jnp.sum(exchanged[:, :rows], axis=0).reshape(shape)
    dots = sum_of_pieces(exchanged[:, rows:], lines).reshape(-1, narrow)[:count]
    return image, dots


def inner_local(first, second):
    totals = jnp.sum(first * second, axis=(0, 1))
    width = totals.shape[0] // 2
    return totals[:width] + totals[width:]


def spread(values):
    return jnp.concatenate([values, values])


def least_squares(hessen, beta):
    gram = [
        [sum(a * b for a, b in zip(hessen[row], hessen[column])) for column in range(row + 1)]
        for row in range(BASIS)
    ]
    factor = [[None] * BASIS for _ in range(BASIS)]
    inverse = [None] * BASIS
    for row in range(BASIS):
        for column in range(row):
            rest = gram[row][column]
            for k in range(column):
                rest = rest - factor[row][k] * factor[column][k]
            factor[row][column] = rest * inverse[column]
        rest = gram[row][row]
        for k in range(row):
            rest = rest - factor[row][k] * factor[row][k]
        factor[row][row] = jnp.sqrt(rest)
        inverse[row] = 1.0 / factor[row][row]
    forward = []
    for row in range(BASIS):
        rest = beta * hessen[row][0]
        for k in range(row):
            rest = rest - factor[row][k] * forward[k]
        forward.append(rest * inverse[row])
    weights = [None] * BASIS
    for row in reversed(range(BASIS)):
        rest = forward[row]
        for k in range(row + 1, BASIS):
            rest = rest - factor[k][row] * weights[k]
        weights[row] = rest * inverse[row]
    return weights


def body(double_layer, single_layer, hypersingular, adjoint_double, matching, right_side, start):
    tile = tile_of_operators(
        double_layer[0], single_layer[0], hypersingular[0], adjoint_double[0]
    )
    right_local = inward(right_side)
    start_local = inward(start)
    selector = selectors(matching, right_local.shape[1])
    start_image = preconditioned(tile, selector, start_local)
    residual = right_local - start_image
    local_dots = jnp.stack(
        [
            inner_local(residual, residual),
            inner_local(start_local, start_image),
            inner_local(start_local, start_local),
        ]
    )
    applied, sums = preconditioned(tile, selector, residual, local_dots)
    beta = jnp.sqrt(sums[0] + EPSILON)
    shift = sums[1] / (sums[2] + EPSILON)
    basis = [residual / spread(beta)]
    images = [applied / spread(beta)]
    gram = (sums[0] / (beta * beta))[None, None]
    hessen = []
    for column in range(BASIS):
        ahead = images[column] - spread(shift) * basis[column]
        local_dots = [inner_local(vector, ahead) for vector in basis]
        local_dots = jnp.stack(local_dots + [inner_local(ahead, ahead)])
        ahead, local_dots, gram, shift, hessen, beta = lax.optimization_barrier(
            (ahead, local_dots, gram, shift, hessen, beta)
        )
        if column + 1 < BASIS:
            applied, sums = preconditioned(tile, selector, ahead, local_dots)
        else:
            sums = summed_everywhere(local_dots)
        dots = sums[: column + 1]
        coefficients = dots + shift * gram[:, column]
        removed = jnp.concatenate([coefficients[:column], dots[column:] + shift * (gram[column:, column] - 1.0)])
        overlaps = jnp.sum(gram * removed[None], axis=1)
        squares = jnp.maximum(
            sums[column + 1] - jnp.sum(removed * (2.0 * dots - overlaps), axis=0), 0.0
        )
        height = jnp.sqrt(squares + EPSILON)
        if column + 1 < BASIS:
            following = ahead
            for earlier in range(column + 1):
                following = following - spread(removed[earlier]) * basis[earlier]
                applied = applied - spread(removed[earlier]) * images[earlier]
            basis.append(following / spread(height))
            images.append(applied / spread(height))
            side = (dots - overlaps) / height
            corner = squares / (height * height)
            gram = jnp.concatenate(
                [
                    jnp.concatenate([gram, side[:, None]], axis=1),
                    jnp.concatenate([side, corner[None]])[None],
                ]
            )
            shift = coefficients[column]
        filler = [jnp.zeros_like(height)] * (BASIS - 1 - column)
        hessen.append([coefficients[earlier] for earlier in range(column + 1)] + [height] + filler)
    weights = least_squares(hessen, beta)
    solution = start_local
    for column in range(BASIS):
        solution = solution + spread(weights[column]) * basis[column]
    return outward(solution)


def solution(mesh):
    torus = Mesh(mesh.devices.reshape(8, 2, 4, 8), ("sub_0", "sub_1", "blk_0", "blk_1"))
    placed = (
        P(SUB, None, BLK, None),
        P(SUB, None, BLK, None),
        P(SUB, None, BLK, None),
        P(SUB, None, BLK, None),
        P(),
        P(SUB, None, None, BLK, None),
        P(SUB, None, None, BLK, None),
    )
    return jax.shard_map(
        body, mesh=torus, in_specs=placed, out_specs=P(SUB, None, None, BLK, None), check_vma=False
    )
```

```python
import jax
import jax.numpy as jnp
from jax import lax
from jax.sharding import Mesh
from jax.sharding import PartitionSpec as P

BASIS = 5
SUB = ("sub_0", "sub_1")
BLK = ("blk_0", "blk_1")


EPSILON = 1e-06


def passed_along(block, axis, distance):
    devices = range(lax.axis_size(axis))
    route = [(i - distance, i) for i in devices if i - distance in devices]
    return lax.ppermute(block, axis, route)


def copy_for_each(value, axis):
    peers = lax.axis_size(axis)
    return lax.all_to_all(
        jnp.broadcast_to(value[None], (peers, *value.shape)), axis, 0, 0, tiled=True
    )


def summed_over(value, axis):
    return jnp.sum(copy_for_each(value, axis), axis=0)


def summed_everywhere(value):
    return summed_over(summed_over(value, SUB), BLK)


def inward(field):
    local_field = field[0]
    return jnp.concatenate([local_field[:, 0], local_field[:, 1]], axis=-1)


def outward(vector):
    width = vector.shape[-1] // 2
    return jnp.stack([vector[..., :width], vector[..., width:]], axis=1)[None]


def tile_of_operators(double_layer, single_layer, hypersingular, adjoint_double):
    columns = lax.axis_size("blk_0")
    grid = ((-double_layer, single_layer), (hypersingular, adjoint_double))
    traces = []
    for line in grid:
        pieces = []
        for part in range(2):
            for operator in line:
                rows, full = operator[part].shape
                pieces.append(
                    jnp.moveaxis(operator[part].reshape(rows, columns, full // columns), 1, 0)
                )
        traces.append(jnp.concatenate(pieces, axis=-1))
    strips = jnp.concatenate(traces, axis=1)
    blocks = lax.all_to_all(strips, "blk_0", 0, 0, tiled=True)
    return blocks.reshape(-1, blocks.shape[-1])


def selectors(matching, local_rows):
    subdomains = lax.axis_size(SUB)
    lines = lax.axis_size("blk_0")
    own_index = lax.axis_index(SUB)
    above_index = jnp.minimum(own_index + 1, subdomains - 1)
    perm_here = lax.dynamic_index_in_dim(matching, own_index, 0, keepdims=False)
    perm_above = lax.dynamic_index_in_dim(matching, above_index, 0, keepdims=False)
    half_rows = local_rows // 2
    half = perm_here.shape[0]
    spots = jnp.arange(half, dtype=jnp.int32)

    def window(values):
        table = values.reshape(lines, lax.axis_size("blk_1"), half_rows)
        return lax.dynamic_index_in_dim(
            table, lax.axis_index("blk_1"), 1, keepdims=False
        ).reshape(-1)

    wanted = window(spots)
    inverse_here = jnp.sum(
        jnp.where(perm_here[None, :] == wanted[:, None], spots[None, :], 0), axis=1
    )
    dofs = jnp.concatenate([2 * window(perm_above) + 1, 2 * inverse_here])
    width = 2 * half // lines
    columns = lax.axis_index("blk_0") * width + jnp.arange(width, dtype=jnp.int32)
    return (dofs[:, None] == columns[None, :]).astype(jnp.bfloat16)


def side_by_side(blocks):
    count, rows, width = blocks.shape
    return jnp.moveaxis(blocks.reshape(count, 2, rows // 2, width), 0, 1).reshape(
        2, count * rows // 2, width
    )


def partial_products(tile, columns):
    width = columns.shape[-1] // 2
    turned = jnp.concatenate([-columns[..., width:], columns[..., :width]], axis=-1)
    stacked = jnp.stack([columns, turned]).reshape(tile.shape[1], 2 * width)
    products = jnp.dot(tile, stacked, preferred_element_type=jnp.float32)
    return products.reshape(lax.axis_size("blk_0"), -1, 2 * width)


def coupling_partials(selector, columns):
    lines = lax.axis_size("blk_0")
    chosen = jnp.einsum(
        "sk,tkn->tsn", selector, columns, preferred_element_type=jnp.float32
    ).astype(jnp.bfloat16)
    middle = chosen.shape[1] // 2
    lower_face = passed_along(chosen[:, :middle], SUB, 1)
    upper_face = passed_along(chosen[:, middle:], SUB, -1)
    joined = jnp.stack([lower_face, upper_face], axis=2)
    joined = joined.reshape(2, lines, 2 * middle // lines, chosen.shape[-1])
    signs = jnp.array([1.0, -1.0], jnp.float32).reshape(1, 2, 1, 1)
    signed = jnp.moveaxis(joined, 1, 0).astype(jnp.float32) * signs
    return signed.reshape(lines, -1, signed.shape[-1])


def exchanged_rows(partials):
    return lax.all_to_all(partials, "blk_0", 0, 0, tiled=True).astype(jnp.float32)


def reduced_rows(partials):
    return jnp.sum(exchanged_rows(partials.astype(jnp.bfloat16)), axis=0)


def padded_rows(value, multiple):
    missing = -value.shape[0] % multiple
    return jnp.pad(value, ((0, missing), (0, 0)))


def in_three_pieces(value):
    high = lax.reduce_precision(value, 8, 7)
    middle = lax.reduce_precision(value - high, 8, 7)
    low = lax.reduce_precision(value - high - middle, 8, 7)
    return jnp.concatenate([high, middle, low]).astype(jnp.bfloat16)


def pieces_of(dots, width):
    packed = padded_rows(dots, 2).reshape(-1, width)
    return padded_rows(in_three_pieces(packed), 16)


def sum_of_pieces(blocks, lines):
    carried = blocks[:, : 3 * lines].astype(jnp.float32)
    return jnp.sum(carried.reshape(-1, 3, lines, carried.shape[-1]), axis=(0, 1))


def preconditioned(tile, selector, vector, dots=None):
    shape = vector.shape
    width = shape[-1]
    payload = vector.astype(jnp.bfloat16).reshape(-1, width)
    rows = payload.shape[0]
    if dots is not None:
        payload, dots = lax.optimization_barrier((payload, dots))
    blocks = copy_for_each(payload, "blk_1")
    if dots is not None:
        blocks, dots = lax.optimization_barrier((blocks, dots))
        dots = summed_over(dots, SUB)
    columns = side_by_side(blocks)
    first = partial_products(tile, columns) - 0.5 * coupling_partials(selector, columns)
    first = first.astype(jnp.bfloat16)
    if dots is None:
        middle = reduced_rows(first).astype(jnp.bfloat16)
        middle_columns = side_by_side(copy_for_each(middle, "blk_1"))
        return reduced_rows(partial_products(tile, middle_columns)).reshape(shape)
    count, narrow = dots.shape
    pieces = pieces_of(dots, width)
    lines = -(-count * narrow // width)
    first, pieces = lax.optimization_barrier((first, pieces))
    middle = reduced_rows(first).astype(jnp.bfloat16)
    blocks = copy_for_each(jnp.concatenate([middle, pieces]), "blk_1")
    second = partial_products(tile, side_by_side(blocks[:, :rows])).astype(jnp.bfloat16)
    carried = in_three_pieces(sum_of_pieces(blocks[:, rows:], lines))
    carried = padded_rows(carried, 16)
    carried = jnp.broadcast_to(carried[None], (second.shape[0], *carried.shape))
    exchanged = exchanged_rows(jnp.concatenate([second, carried], axis=1))
    image = jnp.sum(exchanged[:, :rows], axis=0).reshape(shape)
    dots = sum_of_pieces(exchanged[:, rows:], lines).reshape(-1, narrow)[:count]
    return image, dots


def inner_local(first, second):
    totals = jnp.sum(first * second, axis=(0, 1))
    width = totals.shape[0] // 2
    return totals[:width] + totals[width:]


def spread(values):
    return jnp.concatenate([values, values])


def least_squares(hessen, beta):
    gram = [
        [sum(a * b for a, b in zip(hessen[row], hessen[column])) for column in range(row + 1)]
        for row in range(BASIS)
    ]
    factor = [[None] * BASIS for _ in range(BASIS)]
    inverse = [None] * BASIS
    for row in range(BASIS):
        for column in range(row):
            rest = gram[row][column]
            for k in range(column):
                rest = rest - factor[row][k] * factor[column][k]
            factor[row][column] = rest * inverse[column]
        rest = gram[row][row]
        for k in range(row):
            rest = rest - factor[row][k] * factor[row][k]
        factor[row][row] = jnp.sqrt(rest)
        inverse[row] = 1.0 / factor[row][row]
    forward = []
    for row in range(BASIS):
        rest = beta * hessen[row][0]
        for k in range(row):
            rest = rest - factor[row][k] * forward[k]
        forward.append(rest * inverse[row])
    weights = [None] * BASIS
    for row in reversed(range(BASIS)):
        rest = forward[row]
        for k in range(row + 1, BASIS):
            rest = rest - factor[k][row] * weights[k]
        weights[row] = rest * inverse[row]
    return weights


def product_of(first, second, gram):
    total = 0.0
    for i, left in first.items():
        total = total + left * sum(gram[i][k] * right for k, right in second.items())
    return total


def combined(terms):
    total = {}
    for factor, coordinates in terms:
        for i, value in coordinates.items():
            total[i] = total[i] + factor * value if i in total else factor * value
    return total


def arnoldi_step(vectors, image, gram):
    column = [product_of(vector, image, gram) for vector in vectors]
    rest = combined([(1.0, image)] + [(-h, v) for h, v in zip(column, vectors)])
    height = jnp.sqrt(jnp.maximum(product_of(rest, rest, gram), 0.0) + EPSILON)
    inverse = 1.0 / height
    return column, height, {i: value * inverse for i, value in rest.items()}


def spanned(coordinates, vectors):
    total = 0.0
    for i, value in coordinates.items():
        factor = value if isinstance(value, float) else spread(value)
        total = total + factor * vectors[i]
    return total


def completed(known, values, size):
    values = list(values)
    table = [[None] * size for _ in range(size)]
    for i in range(size):
        for k in range(i + 1):
            entry = known[i][k] if i < len(known) else values.pop(0)
            table[i][k] = table[k][i] = entry
    return table


def rows_of_products(vectors, known):
    return [
        inner_local(vectors[i], vectors[k]) for i in range(known, len(vectors)) for k in range(i + 1)
    ]


def body(double_layer, single_layer, hypersingular, adjoint_double, matching, right_side, start):
    tile = tile_of_operators(
        double_layer[0], single_layer[0], hypersingular[0], adjoint_double[0]
    )
    start_local = inward(start)
    selector = selectors(matching, start_local.shape[1])
    start_image = preconditioned(tile, selector, start_local)
    start_image, start_again, right_side = lax.optimization_barrier(
        (start_image, start_local, right_side)
    )
    residual = inward(right_side) - start_image
    dots = jnp.stack(
        [
            inner_local(residual, residual),
            inner_local(start_again, start_image),
            inner_local(start_again, start_again),
        ]
    )
    applied, sums = preconditioned(tile, selector, residual, dots)
    beta = jnp.sqrt(sums[0] + EPSILON)
    shift = sums[1] / (sums[2] + EPSILON)
    inverse = spread(1.0 / beta)
    basis = [residual * inverse]
    image = applied * inverse
    gram = [[sums[0] / (beta * beta)]]
    hessen = []
    for _ in range(BASIS // 2):
        done = len(basis)
        last = done - 1
        wide = spread(shift)
        first = image - wide * basis[last]
        first, basis, hessen, gram, shift, wide, beta = lax.optimization_barrier(
            (first, basis, hessen, gram, shift, wide, beta)
        )
        first_image = preconditioned(tile, selector, first)
        first_image, first, basis = lax.optimization_barrier((first_image, first, basis))
        second = first_image - wide * first
        spanning = basis + [first, second]
        dots = jnp.stack(rows_of_products(spanning, done))
        second_image, sums = preconditioned(tile, selector, second, dots)
        second_image, sums, spanning, hessen, gram, shift = lax.optimization_barrier(
            (second_image, sums, spanning, hessen, gram, shift)
        )
        table = completed(gram, sums, done + 2)
        images = [
            {row: hessen[column][row] for row in range(column + 2)} for column in range(last)
        ]
        images.append({last: shift, done: 1.0})
        images.append({done: shift, done + 1: 1.0})
        vectors = [{i: 1.0} for i in range(done)]
        column, height, following = arnoldi_step(vectors, images[last], table)
        hessen.append(column + [height])
        vectors.append(following)
        image_ahead = combined([(value, images[i]) for i, value in following.items()])
        column, height, following = arnoldi_step(vectors, image_ahead, table)
        hessen.append(column + [height])
        vectors.append(following)
        local_images = [spanned(known, spanning) for known in images]
        local_images.append(second_image)
        image = spanned(following, local_images)
        basis = [spanned(vector, spanning) for vector in vectors]
        gram = [
            [product_of(vectors[i], vectors[k], table) for k in range(i + 1)]
            for i in range(len(vectors))
        ]
        shift = hessen[-1][-2]
    ahead = image - spread(shift) * basis[-1]
    dots = jnp.stack([inner_local(vector, ahead) for vector in basis + [ahead]])
    dots, hessen, gram, shift, beta, start_again, basis = lax.optimization_barrier(
        (dots, hessen, gram, shift, beta, start_again, basis)
    )
    sums = summed_everywhere(dots)
    sums, hessen, gram, shift, beta, start_again, basis = lax.optimization_barrier(
        (sums, hessen, gram, shift, beta, start_again, basis)
    )
    last = len(basis)
    table = completed(gram, sums, last + 1)
    vectors = [{i: 1.0} for i in range(last)]
    column, height, _ = arnoldi_step(vectors, {last - 1: shift, last: 1.0}, table)
    hessen.append(column + [height])
    hessen = [list(column) + [jnp.zeros_like(beta)] * (BASIS + 1 - len(column)) for column in hessen]
    weights = least_squares(hessen, beta)
    solution = start_again
    for vector, weight in zip(basis, weights):
        solution = solution + spread(weight) * vector
    return outward(solution)


def solution(mesh):
    torus = Mesh(mesh.devices.reshape(8, 2, 4, 8), ("sub_0", "sub_1", "blk_0", "blk_1"))
    placed = (
        P(SUB, None, BLK, None),
        P(SUB, None, BLK, None),
        P(SUB, None, BLK, None),
        P(SUB, None, BLK, None),
        P(),
        P(SUB, None, None, BLK, None),
        P(SUB, None, None, BLK, None),
    )
    return jax.shard_map(
        body, mesh=torus, in_specs=placed, out_specs=P(SUB, None, None, BLK, None), check_vma=False
    )
```

```python
import jax
import jax.numpy as jnp
from jax import lax
from jax.sharding import Mesh
from jax.sharding import PartitionSpec as P

BASIS = 5
SUB = ("sub_0", "sub_1")
BLK = ("blk_0", "blk_1")


EPSILON = 1e-06


def passed_along(block, axis, distance):
    devices = range(lax.axis_size(axis))
    route = [(i - distance, i) for i in devices if i - distance in devices]
    return lax.ppermute(block, axis, route)


def copy_for_each(value, axis):
    peers = lax.axis_size(axis)
    return lax.all_to_all(
        jnp.broadcast_to(value[None], (peers, *value.shape)), axis, 0, 0, tiled=True
    )


def summed_over(value, axis):
    return jnp.sum(copy_for_each(value, axis), axis=0)


def padded_rows(value, multiple):
    missing = -value.shape[0] % multiple
    return jnp.pad(value, ((0, missing), (0, 0)))


def folded(dots):
    width = dots.shape[1] // 2
    return dots[:, :width] + dots[:, width:]


def summed_everywhere(dots):
    count = dots.shape[0]
    rows = folded(padded_rows(dots, 16))
    half = rows.shape[0] // 2
    packed = jnp.concatenate([rows[:half], rows[half:]], axis=1)
    packed = summed_over(summed_over(packed, SUB), BLK)
    width = rows.shape[1]
    return jnp.concatenate([packed[:, :width], packed[:, width:]])[:count]


def inward(field):
    local_field = field[0]
    return jnp.concatenate([local_field[:, 0], local_field[:, 1]], axis=-1)


def outward(vector):
    width = vector.shape[-1] // 2
    return jnp.stack([vector[..., :width], vector[..., width:]], axis=1)[None]


def tile_of_operators(double_layer, single_layer, hypersingular, adjoint_double):
    columns = lax.axis_size("blk_0")
    grid = ((-double_layer, single_layer), (hypersingular, adjoint_double))
    traces = []
    for line in grid:
        pieces = []
        for part in range(2):
            for operator in line:
                rows, full = operator[part].shape
                pieces.append(
                    jnp.moveaxis(operator[part].reshape(rows, columns, full // columns), 1, 0)
                )
        traces.append(jnp.concatenate(pieces, axis=-1))
    strips = jnp.concatenate(traces, axis=1)
    blocks = lax.all_to_all(strips, "blk_0", 0, 0, tiled=True)
    return blocks.reshape(-1, blocks.shape[-1])


def selectors(matching, local_rows):
    subdomains = lax.axis_size(SUB)
    lines = lax.axis_size("blk_0")
    own_index = lax.axis_index(SUB)
    above_index = jnp.minimum(own_index + 1, subdomains - 1)
    perm_here = lax.dynamic_index_in_dim(matching, own_index, 0, keepdims=False)
    perm_above = lax.dynamic_index_in_dim(matching, above_index, 0, keepdims=False)
    half_rows = local_rows // 2
    half = perm_here.shape[0]
    spots = jnp.arange(half, dtype=jnp.int32)

    def window(values):
        table = values.reshape(lines, lax.axis_size("blk_1"), half_rows)
        return lax.dynamic_index_in_dim(
            table, lax.axis_index("blk_1"), 1, keepdims=False
        ).reshape(-1)

    wanted = window(spots)
    inverse_here = jnp.sum(
        jnp.where(perm_here[None, :] == wanted[:, None], spots[None, :], 0), axis=1
    )
    dofs = jnp.concatenate([2 * window(perm_above) + 1, 2 * inverse_here])
    width = 2 * half // lines
    columns = lax.axis_index("blk_0") * width + jnp.arange(width, dtype=jnp.int32)
    return (dofs[:, None] == columns[None, :]).astype(jnp.bfloat16)


def side_by_side(blocks):
    count, rows, width = blocks.shape
    return jnp.moveaxis(blocks.reshape(count, 2, rows // 2, width), 0, 1).reshape(
        2, count * rows // 2, width
    )


def partial_products(tile, columns):
    width = columns.shape[-1] // 2
    turned = jnp.concatenate([-columns[..., width:], columns[..., :width]], axis=-1)
    stacked = jnp.stack([columns, turned]).reshape(tile.shape[1], 2 * width)
    products = jnp.dot(tile, stacked, preferred_element_type=jnp.float32)
    return products.reshape(lax.axis_size("blk_0"), -1, 2 * width)


def coupling_partials(selector, columns):
    lines = lax.axis_size("blk_0")
    chosen = jnp.einsum(
        "sk,tkn->tsn", selector, columns, preferred_element_type=jnp.float32
    ).astype(jnp.bfloat16)
    middle = chosen.shape[1] // 2
    lower_face = passed_along(chosen[:, :middle], SUB, 1)
    upper_face = passed_along(chosen[:, middle:], SUB, -1)
    joined = jnp.stack([lower_face, upper_face], axis=2)
    joined = joined.reshape(2, lines, 2 * middle // lines, chosen.shape[-1])
    signs = jnp.array([1.0, -1.0], jnp.float32).reshape(1, 2, 1, 1)
    signed = jnp.moveaxis(joined, 1, 0).astype(jnp.float32) * signs
    return signed.reshape(lines, -1, signed.shape[-1])


def exchanged_rows(partials):
    return lax.all_to_all(partials, "blk_0", 0, 0, tiled=True).astype(jnp.float32)


def reduced_rows(partials):
    return jnp.sum(exchanged_rows(partials.astype(jnp.bfloat16)), axis=0)


def in_three_pieces(value):
    high = lax.reduce_precision(value, 8, 7)
    middle = lax.reduce_precision(value - high, 8, 7)
    low = lax.reduce_precision(value - high - middle, 8, 7)
    return jnp.concatenate([high, middle, low]).astype(jnp.bfloat16)


def sum_of_pieces(blocks, lines):
    carried = blocks[:, : 3 * lines].astype(jnp.float32)
    return jnp.sum(carried.reshape(-1, 3, lines, carried.shape[-1]), axis=(0, 1))


def preconditioned(tile, selector, vector, dots=None):
    shape = vector.shape
    width = shape[-1]
    payload = vector.astype(jnp.bfloat16).reshape(-1, width)
    rows = payload.shape[0]
    if dots is not None:
        payload, dots = lax.optimization_barrier((payload, dots))
    blocks = copy_for_each(payload, "blk_1")
    if dots is not None:
        blocks, dots = lax.optimization_barrier((blocks, dots))
        dots = summed_over(padded_rows(dots, 8), SUB)[: dots.shape[0]]
    columns = side_by_side(blocks)
    products = lax.optimization_barrier(partial_products(tile, columns))
    first = products - 0.5 * coupling_partials(selector, columns)
    first = first.astype(jnp.bfloat16)
    if dots is None:
        middle = reduced_rows(first).astype(jnp.bfloat16)
        middle_columns = side_by_side(copy_for_each(middle, "blk_1"))
        return reduced_rows(partial_products(tile, middle_columns)).reshape(shape)
    lines = dots.shape[0]
    pieces = padded_rows(in_three_pieces(dots), 16)
    first, pieces = lax.optimization_barrier((first, pieces))
    middle = reduced_rows(first).astype(jnp.bfloat16)
    blocks = copy_for_each(jnp.concatenate([middle, pieces]), "blk_1")
    second = partial_products(tile, side_by_side(blocks[:, :rows])).astype(jnp.bfloat16)
    carried = in_three_pieces(sum_of_pieces(blocks[:, rows:], lines))
    carried = padded_rows(carried, 16)
    carried = jnp.broadcast_to(carried[None], (second.shape[0], *carried.shape))
    exchanged = exchanged_rows(jnp.concatenate([second, carried], axis=1))
    image = jnp.sum(exchanged[:, :rows], axis=0).reshape(shape)
    return image, folded(sum_of_pieces(exchanged[:, rows:], lines))


def inner_local(first, second):
    return jnp.sum(first * second, axis=(0, 1))


def spread(values):
    return jnp.concatenate([values, values])


def least_squares(hessen, beta):
    gram = [
        [sum(a * b for a, b in zip(hessen[row], hessen[column])) for column in range(row + 1)]
        for row in range(BASIS)
    ]
    factor = [[None] * BASIS for _ in range(BASIS)]
    inverse = [None] * BASIS
    for row in range(BASIS):
        for column in range(row):
            rest = gram[row][column]
            for k in range(column):
                rest = rest - factor[row][k] * factor[column][k]
            factor[row][column] = rest * inverse[column]
        rest = gram[row][row]
        for k in range(row):
            rest = rest - factor[row][k] * factor[row][k]
        factor[row][row] = jnp.sqrt(rest)
        inverse[row] = 1.0 / factor[row][row]
    forward = []
    for row in range(BASIS):
        rest = beta * hessen[row][0]
        for k in range(row):
            rest = rest - factor[row][k] * forward[k]
        forward.append(rest * inverse[row])
    weights = [None] * BASIS
    for row in reversed(range(BASIS)):
        rest = forward[row]
        for k in range(row + 1, BASIS):
            rest = rest - factor[k][row] * weights[k]
        weights[row] = rest * inverse[row]
    return weights


def product_of(first, second, gram):
    total = 0.0
    for i, left in first.items():
        total = total + left * sum(gram[i][k] * right for k, right in second.items())
    return total


def combined(terms):
    total = {}
    for factor, coordinates in terms:
        for i, value in coordinates.items():
            total[i] = total[i] + factor * value if i in total else factor * value
    return total


def arnoldi_step(vectors, image, gram):
    column = [product_of(vector, image, gram) for vector in vectors]
    rest = combined([(1.0, image)] + [(-h, v) for h, v in zip(column, vectors)])
    height = jnp.sqrt(jnp.maximum(product_of(rest, rest, gram), 0.0) + EPSILON)
    inverse = 1.0 / height
    return column, height, {i: value * inverse for i, value in rest.items()}


def spanned(coordinates, vectors):
    total = 0.0
    for i, value in coordinates.items():
        factor = value if isinstance(value, float) else spread(value)
        total = total + factor * vectors[i]
    return total


def completed(known, values, size):
    values = list(values)
    table = [[None] * size for _ in range(size)]
    for i in range(size):
        for k in range(i + 1):
            entry = known[i][k] if i < len(known) else values.pop(0)
            table[i][k] = table[k][i] = entry
    return table


def rows_of_products(vectors, known):
    return [
        inner_local(vectors[i], vectors[k]) for i in range(known, len(vectors)) for k in range(i + 1)
    ]


def body(double_layer, single_layer, hypersingular, adjoint_double, matching, right_side, start):
    tile = tile_of_operators(
        double_layer[0], single_layer[0], hypersingular[0], adjoint_double[0]
    )
    start_local = inward(start)
    selector = selectors(matching, start_local.shape[1])
    start_image = preconditioned(tile, selector, start_local)
    start_image, start, right_side = lax.optimization_barrier((start_image, start, right_side))
    start_again = inward(start)
    residual = inward(right_side) - start_image
    dots = jnp.stack(
        [
            inner_local(residual, residual),
            inner_local(start_again, start_image),
            inner_local(start_again, start_again),
        ]
    )
    applied, sums = preconditioned(tile, selector, residual, dots)
    beta = jnp.sqrt(sums[0] + EPSILON)
    shift = sums[1] / (sums[2] + EPSILON)
    inverse = spread(1.0 / beta)
    basis = [residual * inverse]
    image = applied * inverse
    gram = [[sums[0] / (beta * beta)]]

    wide = spread(shift)
    first = image - wide * basis[0]
    first, basis, gram, shift, wide, beta = lax.optimization_barrier(
        (first, basis, gram, shift, wide, beta)
    )
    first_image = preconditioned(tile, selector, first)
    first_image, first, basis = lax.optimization_barrier((first_image, first, basis))
    second = first_image - wide * first
    spanning = basis + [first, second]
    dots = jnp.stack(rows_of_products(spanning, 1))
    second_image, sums = preconditioned(tile, selector, second, dots)
    second_image, sums, spanning, gram, shift = lax.optimization_barrier(
        (second_image, sums, spanning, gram, shift)
    )
    table = completed(gram, sums, 3)
    vectors = [{0: 1.0}]
    images = [{0: shift, 1: 1.0}, {1: shift, 2: 1.0}]
    column, height, following = arnoldi_step(vectors, images[0], table)
    hessen = [column + [height]]
    vectors.append(following)
    image_ahead = combined([(value, images[i]) for i, value in following.items()])
    column, height, following = arnoldi_step(vectors, image_ahead, table)
    hessen.append(column + [height])
    vectors.append(following)
    image = spanned(following, [spanned(known, spanning) for known in images] + [second_image])
    basis = [spanned(vector, spanning) for vector in vectors]
    gram = [
        [product_of(vectors[i], vectors[k], table) for k in range(i + 1)] for i in range(3)
    ]

    shift = hessen[1][1]
    growth = jnp.sqrt(sum(value * value for value in hessen[1]))
    wide, narrower = spread(shift), spread(1.0 / growth)
    third = image - wide * basis[2]
    third, basis, hessen, gram, shift, growth, wide, narrower, beta, start_again = (
        lax.optimization_barrier(
            (third, basis, hessen, gram, shift, growth, wide, narrower, beta, start_again)
        )
    )
    third_image = preconditioned(tile, selector, third)
    third_image, third, wide, narrower = lax.optimization_barrier(
        (third_image, third, wide, narrower)
    )
    fourth = (third_image - wide * third) * narrower
    fourth, wide, narrower = lax.optimization_barrier((fourth, wide, narrower))
    fourth_image = preconditioned(tile, selector, fourth)
    fourth_image, fourth, third, basis, wide, narrower = lax.optimization_barrier(
        (fourth_image, fourth, third, basis, wide, narrower)
    )
    fifth = (fourth_image - wide * fourth) * narrower
    spanning = basis + [third, fourth, fifth]
    dots = jnp.stack(rows_of_products(spanning, 3))
    dots, spanning, hessen, gram, shift, growth, beta, start_again = lax.optimization_barrier(
        (dots, spanning, hessen, gram, shift, growth, beta, start_again)
    )
    sums = summed_everywhere(dots)
    sums, spanning, hessen, gram, shift, growth, beta, start_again = lax.optimization_barrier(
        (sums, spanning, hessen, gram, shift, growth, beta, start_again)
    )
    table = completed(gram, sums, 6)
    images = [
        dict(enumerate(hessen[0])),
        dict(enumerate(hessen[1])),
        {2: shift, 3: 1.0},
        {3: shift, 4: growth},
        {4: shift, 5: growth},
    ]
    vectors = [{i: 1.0} for i in range(3)]
    while len(hessen) < BASIS:
        image_ahead = combined([(value, images[i]) for i, value in vectors[-1].items()])
        column, height, following = arnoldi_step(vectors, image_ahead, table)
        hessen.append(column + [height])
        if len(hessen) < BASIS:
            vectors.append(following)
    hessen = [list(column) + [jnp.zeros_like(beta)] * (BASIS + 1 - len(column)) for column in hessen]
    weights = least_squares(hessen, beta)
    mixture = combined(list(zip(weights, vectors)))
    solution = start_again + spanned(mixture, spanning)
    return outward(solution)


def solution(mesh):
    torus = Mesh(mesh.devices.reshape(8, 2, 4, 8), ("sub_0", "sub_1", "blk_0", "blk_1"))
    placed = (
        P(SUB, None, BLK, None),
        P(SUB, None, BLK, None),
        P(SUB, None, BLK, None),
        P(SUB, None, BLK, None),
        P(),
        P(SUB, None, None, BLK, None),
        P(SUB, None, None, BLK, None),
    )
    return jax.shard_map(
        body, mesh=torus, in_specs=placed, out_specs=P(SUB, None, None, BLK, None), check_vma=False
    )
```

```python
import jax
import jax.numpy as jnp
from jax import lax
from jax.sharding import Mesh
from jax.sharding import PartitionSpec as P

BASIS = 5
SUB = ("sub_0", "sub_1")
BLK = ("blk_0", "blk_1")


EPSILON = 1e-06


def passed_along(block, axis, distance):
    devices = range(lax.axis_size(axis))
    route = [(i - distance, i) for i in devices if i - distance in devices]
    return lax.ppermute(block, axis, route)


def copy_for_each(value, axis):
    peers = lax.axis_size(axis)
    return lax.all_to_all(
        jnp.broadcast_to(value[None], (peers, *value.shape)), axis, 0, 0, tiled=True
    )


def summed_over(value, axis):
    return jnp.sum(copy_for_each(value, axis), axis=0)


def padded_rows(value, multiple):
    missing = -value.shape[0] % multiple
    return jnp.pad(value, ((0, missing), (0, 0)))


def folded(dots):
    width = dots.shape[1] // 2
    return dots[:, :width] + dots[:, width:]


def summed_everywhere(dots):
    count = dots.shape[0]
    rows = folded(padded_rows(dots, 16))
    half = rows.shape[0] // 2
    packed = jnp.concatenate([rows[:half], rows[half:]], axis=1)
    packed = summed_over(summed_over(packed, SUB), BLK)
    width = rows.shape[1]
    return jnp.concatenate([packed[:, :width], packed[:, width:]])[:count]


def inward(field):
    local_field = field[0]
    return jnp.concatenate([local_field[:, 0], local_field[:, 1]], axis=-1)


def outward(vector):
    width = vector.shape[-1] // 2
    return jnp.stack([vector[..., :width], vector[..., width:]], axis=1)[None]


def tile_of_operators(double_layer, single_layer, hypersingular, adjoint_double):
    columns = lax.axis_size("blk_0")
    grid = ((-double_layer, single_layer), (hypersingular, adjoint_double))
    traces = []
    for line in grid:
        pieces = []
        for part in range(2):
            for operator in line:
                rows, full = operator[part].shape
                pieces.append(
                    jnp.moveaxis(operator[part].reshape(rows, columns, full // columns), 1, 0)
                )
        traces.append(jnp.concatenate(pieces, axis=-1))
    strips = jnp.concatenate(traces, axis=1)
    blocks = lax.all_to_all(strips, "blk_0", 0, 0, tiled=True)
    tile = blocks.reshape(-1, blocks.shape[-1])
    half = tile.shape[1] // 2
    return lax.optimization_barrier((tile[:, :half], tile[:, half:]))


def selectors(matching, local_rows):
    subdomains = lax.axis_size(SUB)
    lines = lax.axis_size("blk_0")
    own_index = lax.axis_index(SUB)
    above_index = jnp.minimum(own_index + 1, subdomains - 1)
    perm_here = lax.dynamic_index_in_dim(matching, own_index, 0, keepdims=False)
    perm_above = lax.dynamic_index_in_dim(matching, above_index, 0, keepdims=False)
    half_rows = local_rows // 2
    half = perm_here.shape[0]
    spots = jnp.arange(half, dtype=jnp.int32)

    def window(values):
        table = values.reshape(lines, lax.axis_size("blk_1"), half_rows)
        return lax.dynamic_index_in_dim(
            table, lax.axis_index("blk_1"), 1, keepdims=False
        ).reshape(-1)

    wanted = window(spots)
    inverse_here = jnp.sum(
        jnp.where(perm_here[None, :] == wanted[:, None], spots[None, :], 0), axis=1
    )
    dofs = jnp.concatenate([2 * window(perm_above) + 1, 2 * inverse_here])
    width = 2 * half // lines
    columns = lax.axis_index("blk_0") * width + jnp.arange(width, dtype=jnp.int32)
    return (dofs[:, None] == columns[None, :]).astype(jnp.bfloat16)


def side_by_side(blocks):
    count, rows, width = blocks.shape
    return jnp.moveaxis(blocks.reshape(count, 2, rows // 2, width), 0, 1).reshape(
        2, count * rows // 2, width
    )


def quarter_turn(width):
    lanes = jnp.arange(width, dtype=jnp.int32)
    source, target = lanes[:, None], lanes[None, :]
    half = width // 2
    plus = (source + half == target).astype(jnp.bfloat16)
    minus = (source == target + half).astype(jnp.bfloat16)
    return plus - minus


def partial_products(tile, columns):
    width = columns.shape[-1]
    stacked = columns.reshape(-1, width)
    turned = jnp.dot(
        stacked, quarter_turn(width), preferred_element_type=jnp.float32
    ).astype(jnp.bfloat16)
    real, imaginary = tile
    products = jnp.dot(real, stacked, preferred_element_type=jnp.float32)
    products = products + jnp.dot(imaginary, turned, preferred_element_type=jnp.float32)
    return products.reshape(lax.axis_size("blk_0"), -1, width)


def coupling_partials(selector, columns):
    lines = lax.axis_size("blk_0")
    chosen = jnp.einsum(
        "sk,tkn->tsn", selector, columns, preferred_element_type=jnp.float32
    ).astype(jnp.bfloat16)
    middle = chosen.shape[1] // 2
    lower_face = passed_along(chosen[:, :middle], SUB, 1)
    upper_face = passed_along(chosen[:, middle:], SUB, -1)
    joined = jnp.stack([lower_face, upper_face], axis=2)
    joined = joined.reshape(2, lines, 2 * middle // lines, chosen.shape[-1])
    signs = jnp.array([1.0, -1.0], jnp.float32).reshape(1, 2, 1, 1)
    signed = jnp.moveaxis(joined, 1, 0).astype(jnp.float32) * signs
    return signed.reshape(lines, -1, signed.shape[-1])


def exchanged_rows(partials):
    return lax.all_to_all(partials, "blk_0", 0, 0, tiled=True).astype(jnp.float32)


def reduced_rows(partials):
    return jnp.sum(exchanged_rows(partials.astype(jnp.bfloat16)), axis=0)


def in_three_pieces(value):
    high = lax.reduce_precision(value, 8, 7)
    middle = lax.reduce_precision(value - high, 8, 7)
    low = lax.reduce_precision(value - high - middle, 8, 7)
    return jnp.concatenate([high, middle, low]).astype(jnp.bfloat16)


def sum_of_pieces(blocks, lines):
    carried = blocks[:, : 3 * lines].astype(jnp.float32)
    return jnp.sum(carried.reshape(-1, 3, lines, carried.shape[-1]), axis=(0, 1))


def preconditioned(tile, selector, vector, dots=None):
    shape = vector.shape
    width = shape[-1]
    payload = vector.astype(jnp.bfloat16).reshape(-1, width)
    rows = payload.shape[0]
    if dots is not None:
        payload, dots = lax.optimization_barrier((payload, dots))
    blocks = copy_for_each(payload, "blk_1")
    if dots is not None:
        blocks, dots = lax.optimization_barrier((blocks, dots))
        dots = summed_over(padded_rows(dots, 8), SUB)[: dots.shape[0]]
    columns = side_by_side(blocks)
    products = lax.optimization_barrier(partial_products(tile, columns))
    first = products - 0.5 * coupling_partials(selector, columns)
    first = first.astype(jnp.bfloat16)
    if dots is None:
        middle = reduced_rows(first).astype(jnp.bfloat16)
        middle_columns = side_by_side(copy_for_each(middle, "blk_1"))
        return reduced_rows(partial_products(tile, middle_columns)).reshape(shape)
    lines = dots.shape[0]
    pieces = padded_rows(in_three_pieces(dots), 16)
    first, pieces = lax.optimization_barrier((first, pieces))
    middle = reduced_rows(first).astype(jnp.bfloat16)
    blocks = copy_for_each(jnp.concatenate([middle, pieces]), "blk_1")
    second = partial_products(tile, side_by_side(blocks[:, :rows])).astype(jnp.bfloat16)
    carried = in_three_pieces(sum_of_pieces(blocks[:, rows:], lines))
    carried = padded_rows(carried, 16)
    carried = jnp.broadcast_to(carried[None], (second.shape[0], *carried.shape))
    exchanged = exchanged_rows(jnp.concatenate([second, carried], axis=1))
    image = jnp.sum(exchanged[:, :rows], axis=0).reshape(shape)
    return image, folded(sum_of_pieces(exchanged[:, rows:], lines))


def inner_local(first, second):
    return jnp.sum(first * second, axis=(0, 1))


def spread(values):
    return jnp.concatenate([values, values])


def least_squares(hessen, beta):
    gram = [
        [sum(a * b for a, b in zip(hessen[row], hessen[column])) for column in range(row + 1)]
        for row in range(BASIS)
    ]
    factor = [[None] * BASIS for _ in range(BASIS)]
    inverse = [None] * BASIS
    for row in range(BASIS):
        for column in range(row):
            rest = gram[row][column]
            for k in range(column):
                rest = rest - factor[row][k] * factor[column][k]
            factor[row][column] = rest * inverse[column]
        rest = gram[row][row]
        for k in range(row):
            rest = rest - factor[row][k] * factor[row][k]
        factor[row][row] = jnp.sqrt(rest)
        inverse[row] = 1.0 / factor[row][row]
    forward = []
    for row in range(BASIS):
        rest = beta * hessen[row][0]
        for k in range(row):
            rest = rest - factor[row][k] * forward[k]
        forward.append(rest * inverse[row])
    weights = [None] * BASIS
    for row in reversed(range(BASIS)):
        rest = forward[row]
        for k in range(row + 1, BASIS):
            rest = rest - factor[k][row] * weights[k]
        weights[row] = rest * inverse[row]
    return weights


def product_of(first, second, gram):
    total = 0.0
    for i, left in first.items():
        total = total + left * sum(gram[i][k] * right for k, right in second.items())
    return total


def combined(terms):
    total = {}
    for factor, coordinates in terms:
        for i, value in coordinates.items():
            total[i] = total[i] + factor * value if i in total else factor * value
    return total


def arnoldi_step(vectors, image, gram):
    column = [product_of(vector, image, gram) for vector in vectors]
    rest = combined([(1.0, image)] + [(-h, v) for h, v in zip(column, vectors)])
    height = jnp.sqrt(jnp.maximum(product_of(rest, rest, gram), 0.0) + EPSILON)
    inverse = 1.0 / height
    return column, height, {i: value * inverse for i, value in rest.items()}


def spanned(coordinates, vectors):
    total = 0.0
    for i, value in coordinates.items():
        factor = value if isinstance(value, float) else spread(value)
        total = total + factor * vectors[i]
    return total


def completed(known, values, size):
    values = list(values)
    table = [[None] * size for _ in range(size)]
    for i in range(size):
        for k in range(i + 1):
            entry = known[i][k] if i < len(known) else values.pop(0)
            table[i][k] = table[k][i] = entry
    return table


def rows_of_products(vectors, known):
    return [
        inner_local(vectors[i], vectors[k]) for i in range(known, len(vectors)) for k in range(i + 1)
    ]


def body(double_layer, single_layer, hypersingular, adjoint_double, matching, right_side, start):
    tile = tile_of_operators(
        double_layer[0], single_layer[0], hypersingular[0], adjoint_double[0]
    )
    start_local = inward(start)
    selector = selectors(matching, start_local.shape[1])
    start_image = preconditioned(tile, selector, start_local)
    start_image, start, right_side = lax.optimization_barrier((start_image, start, right_side))
    start_again = inward(start)
    residual = inward(right_side) - start_image
    dots = jnp.stack(
        [
            inner_local(residual, residual),
            inner_local(start_again, start_image),
            inner_local(start_again, start_again),
        ]
    )
    applied, sums = preconditioned(tile, selector, residual, dots)
    beta = jnp.sqrt(sums[0] + EPSILON)
    shift = sums[1] / (sums[2] + EPSILON)
    inverse = spread(1.0 / beta)
    basis = [residual * inverse]
    image = applied * inverse
    gram = [[sums[0] / (beta * beta)]]

    wide = spread(shift)
    first = image - wide * basis[0]
    first, basis, gram, shift, wide, beta = lax.optimization_barrier(
        (first, basis, gram, shift, wide, beta)
    )
    first_image = preconditioned(tile, selector, first)
    first_image, first, basis = lax.optimization_barrier((first_image, first, basis))
    second = first_image - wide * first
    spanning = basis + [first, second]
    dots = jnp.stack(rows_of_products(spanning, 1))
    second_image, sums = preconditioned(tile, selector, second, dots)
    second_image, sums, spanning, gram, shift = lax.optimization_barrier(
        (second_image, sums, spanning, gram, shift)
    )
    table = completed(gram, sums, 3)
    vectors = [{0: 1.0}]
    images = [{0: shift, 1: 1.0}, {1: shift, 2: 1.0}]
    column, height, following = arnoldi_step(vectors, images[0], table)
    hessen = [column + [height]]
    vectors.append(following)
    image_ahead = combined([(value, images[i]) for i, value in following.items()])
    column, height, following = arnoldi_step(vectors, image_ahead, table)
    hessen.append(column + [height])
    vectors.append(following)
    image = spanned(following, [spanned(known, spanning) for known in images] + [second_image])
    basis = [spanned(vector, spanning) for vector in vectors]
    gram = [
        [product_of(vectors[i], vectors[k], table) for k in range(i + 1)] for i in range(3)
    ]

    shift = hessen[1][1]
    growth = jnp.sqrt(sum(value * value for value in hessen[1]))
    wide, narrower = spread(shift), spread(1.0 / growth)
    third = image - wide * basis[2]
    third, basis, hessen, gram, shift, growth, wide, narrower, beta, start_again = (
        lax.optimization_barrier(
            (third, basis, hessen, gram, shift, growth, wide, narrower, beta, start_again)
        )
    )
    third_image = preconditioned(tile, selector, third)
    third_image, third, wide, narrower = lax.optimization_barrier(
        (third_image, third, wide, narrower)
    )
    fourth = (third_image - wide * third) * narrower
    fourth, wide, narrower = lax.optimization_barrier((fourth, wide, narrower))
    fourth_image = preconditioned(tile, selector, fourth)
    fourth_image, fourth, third, basis, wide, narrower = lax.optimization_barrier(
        (fourth_image, fourth, third, basis, wide, narrower)
    )
    fifth = (fourth_image - wide * fourth) * narrower
    spanning = basis + [third, fourth, fifth]
    dots = jnp.stack(rows_of_products(spanning, 3))
    dots, spanning, hessen, gram, shift, growth, beta, start_again = lax.optimization_barrier(
        (dots, spanning, hessen, gram, shift, growth, beta, start_again)
    )
    sums = summed_everywhere(dots)
    sums, spanning, hessen, gram, shift, growth, beta, start_again = lax.optimization_barrier(
        (sums, spanning, hessen, gram, shift, growth, beta, start_again)
    )
    table = completed(gram, sums, 6)
    images = [
        dict(enumerate(hessen[0])),
        dict(enumerate(hessen[1])),
        {2: shift, 3: 1.0},
        {3: shift, 4: growth},
        {4: shift, 5: growth},
    ]
    vectors = [{i: 1.0} for i in range(3)]
    while len(hessen) < BASIS:
        image_ahead = combined([(value, images[i]) for i, value in vectors[-1].items()])
        column, height, following = arnoldi_step(vectors, image_ahead, table)
        hessen.append(column + [height])
        if len(hessen) < BASIS:
            vectors.append(following)
    hessen = [list(column) + [jnp.zeros_like(beta)] * (BASIS + 1 - len(column)) for column in hessen]
    weights = least_squares(hessen, beta)
    mixture = combined(list(zip(weights, vectors)))
    solution = start_again + spanned(mixture, spanning)
    return outward(solution)


def solution(mesh):
    torus = Mesh(mesh.devices.reshape(8, 2, 4, 8), ("sub_0", "sub_1", "blk_0", "blk_1"))
    placed = (
        P(SUB, None, BLK, None),
        P(SUB, None, BLK, None),
        P(SUB, None, BLK, None),
        P(SUB, None, BLK, None),
        P(),
        P(SUB, None, None, BLK, None),
        P(SUB, None, None, BLK, None),
    )
    return jax.shard_map(
        body, mesh=torus, in_specs=placed, out_specs=P(SUB, None, None, BLK, None), check_vma=False
    )
```
